256 devices in a mesh: engine: 4 (over y), ep: 64 (over x, z, core).
Axes of the slice: x: 4, y: 4, z: 8, core: 2. Of those that a mesh axis runs over, the one named last changes fastest.
Arguments:
- tokens: bfloat16 [2, 2048, 4096], P(None, ('engine', 'ep')), may hold values from -6 to 6
- route_ids: int32 [2, 2048, 8], P(None, ('engine', 'ep')), may hold values from 0 to 63, all different within a row; in each aligned block of 8 rows (0 to 7, 8 to 15, ..., all dimensions but the last counted through in order) at most 2 rows name the same one
- route_weights: float32 [2, 2048, 8], P(None, ('engine', 'ep')), may hold values from 0.05 to 1
- placement: int32 [64], replicated, may hold values from 0 to 63, each once
- expert_in: bfloat16 [64, 2, 4096, 1536], P(None, None, ('engine', 'ep')), may hold values from -0.09375 to 0.09375
- expert_down: bfloat16 [64, 1536, 4096], P(None, None, ('engine', 'ep')), may hold values from -0.15625 to 0.15625
Outputs:
- combined: bfloat16 [2, 2048, 4096], P(None, ('engine', 'ep'))
- in_scales: float32 [64, 2, 1536], P('ep', None, 'engine')
- out_scales: float32 [64, 4096], P('ep', 'engine')
The draws below stay inside these ranges and needn't reach their ends.
Inputs may be any that keep to these rules, and one draw needn't show every extreme that they name: `route_ids`: within the rows of one device in one step no expert is named more than 2 times, a bound that some block reaches. `placement`: each slot holds exactly one expert.
All inputs are finite; a program needn't handle non-finite values.
Results may differ from the reference program's by a relative error of at most 0.0057.
Values may be sent and summed in bfloat16 or wider, within the bound.
A program may use at most 128 MiB of HBM per device.

```python
import math
import jax
import jax.numpy as jnp
import numpy as np
from jax import lax

D = 4096
FF = 1536
TOP = 8
STEPS = 2
TOK_DEV = 8
EXPERTS = 64
MOST = 2
TOKENS = 2048


def shard_levels(own_key, extent, pieces, low, top_value):
    def one(position, parts):
        heights = jax.random.uniform(jax.random.fold_in(jax.random.fold_in(own_key, 6), position), (parts,), jnp.float32, low / len(pieces), top_value / len(pieces))
        return jnp.repeat(jnp.exp(heights), extent[position] // parts).reshape((-1,) + (1,) * (len(extent) - position - 1))

    level = one(*pieces[0])
    for cut in pieces[1:]:
        level = level * one(*cut)
    return level


def shared_out(key, own, number, rows, number_of, top, bound, lean):
    sequence = jax.random.permutation(key, number_of)
    heavy_load, common = load_shares(number_of, rows * top, bound, lean, True), load_shares(number_of, rows * top, bound, lean, False)
    places = jnp.arange(number_of)

    def named(lengths, turn):
        used = int((lengths > 0).sum())
        fixed = max(1, used // 4)
        passed = fixed + (places - fixed + turn * (used - fixed)) % max(1, number_of - fixed)
        return jnp.zeros((number_of,), jnp.int32).at[sequence[jnp.where(places < fixed, places, passed)]].set(jnp.asarray(lengths, jnp.int32))

    lengths = jnp.where(number % 4 == 0, named(heavy_load, number // 4), named(common, number - number // 4 - 1))
    mixed = jax.random.permutation(jax.random.fold_in(own, 3), number_of)
    donor, taker = mixed[0:number_of // 2 * 2:2], mixed[1:number_of // 2 * 2:2]
    margin = jnp.minimum(lengths[donor] - 1, bound - lengths[taker]) // 2
    margin = jnp.where((donor == sequence[0]) | (taker == sequence[0]) | (lengths[taker] == 0), 0, jnp.maximum(margin, 0))
    passed = jax.random.randint(jax.random.fold_in(own, 4), (number_of // 2,), 0, 1 << 20) % (margin + 1)
    lengths = lengths.at[donor].add(-passed).at[taker].add(passed)
    labels = jnp.searchsorted(jnp.cumsum(lengths), jnp.arange(rows * top), side="right").astype(jnp.int32)
    table = labels.reshape(top, rows).T
    table = table[jax.random.permutation(jax.random.fold_in(own, 1), rows)]
    turn = jax.random.randint(jax.random.fold_in(own, 2), (rows, 1), 0, top)
    return jnp.take_along_axis(table, (jnp.arange(top)[None, :] + turn) % top, axis=1)


def load_shares(count, total, bound, skew, full):
    portions = [(1 << 20) // math.isqrt(grade ** skew) + 1 for grade in range(1, count + 1)]
    largest = bound if full else min(bound, max(-(-total // count), total * portions[0] // sum(portions)))
    least = 1 if total - largest >= count - 1 else 0
    holding, surplus = [largest] + [least] * (count - 1), total - largest - least * (count - 1)
    while surplus > 0:
        free = [i for i in range(1, count) if holding[i] < largest] or [i for i in range(1, count) if holding[i] < bound]
        pool, budget = sum([portions[i] for i in free]), surplus
        for i in free:
            more = min(bound - holding[i], max(1, budget * portions[i] // pool), surplus)
            holding[i] = holding[i] + more
            surplus = surplus - more
    return np.array(holding)


def normal_values(stream_key, dims, scale, most, split=(), kind=jnp.bfloat16):
    loudness = shard_levels(stream_key, dims, split, -0.22, 0.18) if split else 1.0
    values = jax.random.normal(stream_key, dims, jnp.float32) * scale * loudness
    return jnp.minimum(jnp.maximum(values, -most), most).astype(kind)


def setup_inputs(seed: int = 0) -> dict:
    key_of = jax.random.split(jax.random.key(seed), 7)
    tokens = normal_values(key_of[0], (STEPS, TOKENS, D), 1.0, 6.0, ((1, 256),))
    route_ids_keys = jax.random.split(jax.random.fold_in(key_of[1], 1), STEPS * TOKENS // TOK_DEV)
    route_ids_turns = jax.random.permutation(jax.random.fold_in(key_of[1], 3), STEPS * TOKENS // TOK_DEV)
    route_ids = jax.vmap(lambda own, number: shared_out(jax.random.fold_in(key_of[1], 2), own, number, TOK_DEV, EXPERTS, TOP, MOST, 1))(route_ids_keys, route_ids_turns).reshape((STEPS, TOKENS, TOP))
    route_weights = jnp.clip(0.05 + 0.95 * jax.random.uniform(key_of[2], (STEPS, TOKENS, TOP), jnp.float32) ** shard_levels(key_of[2], (STEPS, TOKENS, TOP), ((1, 256),), -0.2, 0.2), 0.05, 1.0)
    placement = jax.random.permutation(key_of[3], EXPERTS).astype(jnp.int32)
    expert_in = normal_values(key_of[4], (EXPERTS, 2, D, FF), D ** -0.5, 0.09375, ((2, 256),))
    expert_down = normal_values(key_of[5], (EXPERTS, FF, D), FF ** -0.5, 0.15625, ((2, 256),))
    return {"tokens": tokens, "route_ids": route_ids, "route_weights": route_weights, "placement": placement, "expert_in": expert_in, "expert_down": expert_down}


EPSILON = 1e-6
quant_levels = 31.0


def reference(tokens, route_ids, route_weights, placement, expert_in, expert_down):
    experts = expert_in.shape[0]
    row_room = (TOKENS // TOK_DEV) * MOST
    positions = jnp.arange(row_room, dtype=jnp.int32)

    def one_expert(running, expert_id):
        weights_in = expert_in[expert_id].astype(jnp.float32)
        weights_down = expert_down[expert_id].astype(jnp.float32)
        scale_in = (jnp.max(jnp.abs(weights_in), axis=1) + EPSILON) / quant_levels
        scale_out = (jnp.max(jnp.abs(weights_down), axis=0) + EPSILON) / quant_levels
        quant_in = jnp.floor(weights_in / scale_in[:, None, :] + 0.5).astype(jnp.bfloat16)
        quant_down = jnp.floor(weights_down / scale_out[None, :] + 0.5).astype(jnp.bfloat16)
        updated = []
        for step_index in range(STEPS):
            matched = route_ids[step_index] == expert_id
            weight_sum = jnp.sum(jnp.where(matched, route_weights[step_index], 0.0), axis=1)
            chosen = jnp.any(matched, axis=1)
            row_ids = jnp.nonzero(chosen, size=row_room, fill_value=0)[0].astype(jnp.int32)
            usable = positions < jnp.sum(chosen.astype(jnp.int32))
            picked = tokens[step_index][row_ids]
            gate_part = jnp.dot(picked, quant_in[0], preferred_element_type=jnp.float32) * scale_in[0]
            up_part = jnp.dot(picked, quant_in[1], preferred_element_type=jnp.float32) * scale_in[1]
            hidden = (jax.nn.silu(gate_part) * up_part).astype(jnp.bfloat16)
            result = (jnp.dot(hidden, quant_down, preferred_element_type=jnp.float32) * scale_out).astype(jnp.bfloat16)
            weight = jnp.where(usable, weight_sum[row_ids], 0.0)
            updated.append(running[step_index].at[row_ids].add(result.astype(jnp.float32) * weight[:, None]))
        return jnp.stack(updated), (scale_in, scale_out)

    initial = jnp.zeros((STEPS, TOKENS, D), jnp.float32)
    summed, scales = lax.scan(one_expert, initial, jnp.arange(experts, dtype=jnp.int32))
    scales_in, scales_out = scales
    slot_in = jnp.zeros_like(scales_in).at[placement].set(scales_in)
    slot_out = jnp.zeros_like(scales_out).at[placement].set(scales_out)
    return summed.astype(jnp.bfloat16), slot_in, slot_out
```

```python
import jax
import jax.numpy as jnp
from jax import lax
from jax.sharding import PartitionSpec as P

EPSILON = 1e-06
quant_levels = 31.0
BOTH = ("engine", "ep")


def first_slots(named, capacity):
    counted = named.astype(jnp.int32)
    before = jnp.cumsum(counted, axis=-2) - counted
    return jnp.stack([named & (before == slot) for slot in range(capacity)], axis=-3)


def shards(tokens, route_ids, route_weights, placement, expert_in, expert_down):
    experts = placement.shape[0]
    engines = lax.axis_size("engine")
    peers = lax.axis_size("ep")
    me = lax.axis_index("ep")
    steps, row_count, width = tokens.shape
    capacity = 2
    hidden_units = expert_in.shape[3]
    units = hidden_units // engines
    shard_rows = expert_in.shape[2]
    numbers = jnp.arange(experts, dtype=jnp.int32)
    mine = jnp.sum(jnp.where(placement == me, numbers, 0))

    ids = jnp.pad(route_ids, ((0, 0), (0, 0), (0, 128 - route_ids.shape[2])), constant_values=-1)
    payload = jnp.concatenate([tokens, ids.astype(jnp.bfloat16)], axis=2)
    everyone = lax.all_gather(payload, "ep", axis=0, tiled=False)

    parts = jnp.concatenate([expert_in[..., e * units : (e + 1) * units] for e in range(engines)], axis=0)
    held_in = lax.all_to_all(parts, BOTH, split_axis=0, concat_axis=0, tiled=True)

    down = jnp.transpose(expert_down, (0, 2, 1))
    down_top = jnp.max(jnp.abs(down), axis=2).astype(jnp.float32)
    down_scale = (down_top + EPSILON) / quant_levels
    quant_down = jnp.floor(down.astype(jnp.float32) / down_scale[:, :, None] + 0.5).astype(jnp.bfloat16)
    all_down_scales = lax.all_gather(down_scale, "ep", axis=1, tiled=True)
    held_down = lax.all_to_all(quant_down, "ep", split_axis=0, concat_axis=0, tiled=True)
    scale_out = lax.dynamic_index_in_dim(all_down_scales, me, 0, keepdims=False)
    out_scales = lax.dynamic_index_in_dim(all_down_scales, mine, 0, keepdims=True)

    named = jnp.any(everyone[..., width : width + route_ids.shape[2]] == me.astype(jnp.bfloat16), axis=-1)
    slots = first_slots(named[..., None], capacity)[..., 0]
    same = jnp.eye(peers, dtype=jnp.bool_)
    arrived = []
    for step in range(steps):
        chosen = (slots[:, step, :, None, :] & same[:, None, :, None]).reshape(peers * capacity, peers * row_count)
        rows = everyone[:, step, :, :width].reshape(peers * row_count, width)
        arrived.append(
            jnp.dot(chosen.astype(jnp.bfloat16), rows, preferred_element_type=jnp.float32).astype(jnp.bfloat16)
        )
    arrived = jnp.stack(arrived)
    gathered = lax.all_gather(arrived, "engine", axis=1, tiled=True)

    top = jnp.max(jnp.abs(held_in), axis=(0, 2)).astype(jnp.float32)
    scale_in = (top + EPSILON) / quant_levels
    quant_in = jnp.floor(held_in.astype(jnp.float32) / scale_in[None, :, None, :] + 0.5).astype(jnp.bfloat16)
    quant_in = jnp.transpose(quant_in, (1, 0, 2, 3)).reshape(2, width, units)
    all_in_scales = lax.all_gather(scale_in, "ep", axis=0, tiled=False)
    in_scales = lax.dynamic_index_in_dim(all_in_scales, mine, 0, keepdims=True)
    projected = jnp.einsum("snd,mdf->msnf", gathered, quant_in, preferred_element_type=jnp.float32)
    projected = projected * scale_in[:, None, None, :]
    hidden = (jax.nn.silu(projected[0]) * projected[1]).astype(jnp.bfloat16)
    hidden = lax.all_gather(hidden, "engine", axis=0, tiled=False)
    hidden = jnp.concatenate([hidden[e] for e in range(engines)], axis=-1)
    columns = held_down.reshape(-1, hidden_units)
    summed = jnp.einsum("snf,cf->nsc", hidden, columns, preferred_element_type=jnp.float32)
    outcome = (summed * scale_out.reshape(-1)).astype(jnp.bfloat16)
    outcome = outcome.reshape(engines * peers, capacity, steps, -1)
    returned = lax.all_to_all(outcome, BOTH, split_axis=0, concat_axis=0, tiled=True)
    returned = returned.reshape(engines, peers * capacity, steps, -1)

    wanted = route_ids[..., None] == numbers
    weights = jnp.sum(jnp.where(wanted, route_weights[..., None], 0.0), axis=2)
    filled = first_slots(jnp.any(wanted, axis=2), capacity)
    mixing = jnp.where(filled, weights[:, None], 0.0)
    mixing = jnp.transpose(mixing, (0, 2, 3, 1)).reshape(steps, row_count, peers * capacity)
    combined = jnp.stack(
        [
            jnp.einsum(
                "il,eld->ied", mixing[step], returned[:, :, step].astype(jnp.float32), precision=lax.Precision.HIGHEST
            )
            for step in range(steps)
        ]
    )
    combined = combined.reshape(steps, row_count, width)
    return (combined.astype(jnp.bfloat16), in_scales, out_scales.reshape(1, -1))


def solution(mesh):
    placed = (
        P(None, ("engine", "ep"), None),
        P(None, ("engine", "ep"), None),
        P(None, ("engine", "ep"), None),
        P(),
        P(None, None, ("engine", "ep"), None),
        P(None, None, ("engine", "ep")),
    )
    return jax.shard_map(
        shards,
        mesh=mesh,
        in_specs=placed,
        out_specs=(P(None, ("engine", "ep"), None), P("ep", None, "engine"), P("ep", "engine")),
        check_vma=False,
    )
```

```python
import jax
import jax.numpy as jnp
from jax import lax
from jax.experimental import pallas as pl
from jax.experimental.pallas import tpu as pltpu
from jax.sharding import PartitionSpec as P


EPSILON = 1e-06
quant_levels = 31.0
BOTH = ("engine", "ep")
MESH = pl.DeviceIdType.MESH
XS, ZS, CS, YS = 4, 8, 2, 4


def place():
    p = lax.axis_index("ep")
    return lax.axis_index("engine"), p // (ZS * CS), (p // CS) % ZS, p % CS


def device(y, x, z, c):
    return {"engine": y, "ep": x * (ZS * CS) + z * CS + c}


def peers_of(kind):
    y, x, z, c = place()
    if kind == "z":
        return [device(y, x, (z + d) % ZS, c) for d in (4, 3, 5, 2, 6, 1, 7)]
    if kind == "x":
        return [device(y, (x + d) % XS, z, c) for d in (2, 1, 3)]
    if kind == "y":
        return [device((y + d) % YS, x, z, c) for d in (2, 1, 3)]
    if kind == "c":
        return [device(y, x, z, 1 - c)]
    return [device(y, (x + d) % XS, z, (c + f) % CS) for f in (0, 1) for d in range(XS) if (d, f) != (0, 0)]


def greet(kinds):
    barrier = pltpu.get_barrier_semaphore()
    count = 0
    for kind in kinds:
        for peer in peers_of(kind):
            pl.semaphore_signal(barrier, inc=1, device_id=peer, device_id_type=MESH)
            count += 1
    pl.semaphore_wait(barrier, count)


def send(src, dst, send_sem, recv_sem, peer):
    copy = pltpu.make_async_remote_copy(
        src_ref=src, dst_ref=dst, send_sem=send_sem, recv_sem=recv_sem, device_id=peer, device_id_type=MESH
    )
    copy.start()
    return copy


def await_bytes(like, sem):
    pltpu.make_async_copy(like, like, sem).wait()


def dispatch_kernel(tok_ref, meta_ref, all_tok, plane, cols, sent, got, own):
    y, x, z, c = place()
    greet(("z", "x", "y", "c"))
    mine = pltpu.make_async_copy(tok_ref, all_tok.at[c, x, z], own)
    mine.start()
    for peer in peers_of("z"):
        send(tok_ref, all_tok.at[c, x, z], sent.at[0], got.at[0], peer)
        send(meta_ref, plane.at[c, x, z], sent.at[1], got.at[1], peer)
    plane[c, x, z] = meta_ref[...]
    mine.wait()
    await_bytes(plane.at[c, x, pl.ds(0, ZS - 1)], got.at[1])
    await_bytes(all_tok.at[c, x, pl.ds(0, ZS - 1)], got.at[0])
    for peer in peers_of("x"):
        send(all_tok.at[c, x], all_tok.at[c, x], sent.at[2], got.at[2], peer)
        send(plane.at[c, x], plane.at[c, x], sent.at[3], got.at[3], peer)
    for peer in peers_of("y"):
        send(plane.at[c, x], cols.at[y], sent.at[4], got.at[4], peer)
    cols[y] = plane[c, x]
    await_bytes(plane.at[c, pl.ds(0, XS - 1)], got.at[3])
    await_bytes(all_tok.at[c, pl.ds(0, XS - 1)], got.at[2])
    for peer in peers_of("c"):
        send(all_tok.at[c], all_tok.at[c], sent.at[5], got.at[5], peer)
        send(plane.at[c], plane.at[c], sent.at[6], got.at[6], peer)
    await_bytes(cols.at[pl.ds(0, YS - 1)], got.at[4])
    await_bytes(plane.at[c], got.at[6])
    await_bytes(all_tok.at[c], got.at[5])
    await_bytes(all_tok.at[c, x, pl.ds(0, ZS - 1)], sent.at[0])
    await_bytes(plane.at[c, x, pl.ds(0, ZS - 1)], sent.at[1])
    await_bytes(all_tok.at[c, pl.ds(0, XS - 1)], sent.at[2])
    await_bytes(plane.at[c, pl.ds(0, XS - 1)], sent.at[3])
    await_bytes(cols.at[pl.ds(0, YS - 1)], sent.at[4])
    await_bytes(all_tok.at[c], sent.at[5])
    await_bytes(plane.at[c], sent.at[6])


def dispatch(tok, meta):
    rows, width = tok.shape
    vmem = pl.BlockSpec(memory_space=pltpu.VMEM)
    return pl.pallas_call(
        dispatch_kernel,
        out_shape=(
            jax.ShapeDtypeStruct((CS, XS, ZS, rows, width), tok.dtype),
            jax.ShapeDtypeStruct((CS, XS, ZS) + meta.shape, meta.dtype),
            jax.ShapeDtypeStruct((YS, ZS) + meta.shape, meta.dtype),
        ),
        in_specs=[vmem, vmem],
        out_specs=(pl.BlockSpec(memory_space=pl.ANY), vmem, vmem),
        scratch_shapes=[pltpu.SemaphoreType.DMA((7,)), pltpu.SemaphoreType.DMA((7,)), pltpu.SemaphoreType.DMA],
        compiler_params=pltpu.CompilerParams(collective_id=0, has_side_effects=True),
        cost_estimate=pl.CostEstimate(flops=20_000_000_000, bytes_accessed=10_000_000, transcendentals=0),
        name="dispatch",
    )(tok, meta)


def return_kernel(outcome, mixing, out, first, partial, second, total, third, sent, got, own):
    steps = outcome.shape[0]
    y, x, z, c = place()
    here = c * XS + x
    greet(("xc", "z", "y"))
    locals_ = []
    for s in range(steps):
        local = pltpu.make_async_copy(outcome.at[s, :, here], first.at[s, here], own.at[s])
        local.start()
        locals_.append(local)
        for f, d in ((0, 2), (0, 1), (0, 3), (1, 2), (1, 1), (1, 3), (1, 0)):
            there_x, there_c = (x + d) % XS, (c + f) % CS
            src = outcome.at[s, :, there_c * XS + there_x]
            send(src, first.at[s, here], sent.at[s], got.at[s], device(y, there_x, z, there_c))
    for s in range(steps):
        locals_[s].wait()
        await_bytes(first.at[s, pl.ds(0, XS * CS - 1)], got.at[s])
        rows = first[s].reshape(-1, first.shape[-1]).astype(jnp.float32)
        sums = jnp.dot(mixing[s], rows, precision=lax.Precision.HIGHEST, preferred_element_type=jnp.float32)
        partial[s] = sums.astype(partial.dtype).reshape(partial.shape[1:])
        second[s, z] = partial[s, z]
        for d in (4, 3, 5, 2, 6, 1, 7):
            there = (z + d) % ZS
            send(partial.at[s, there], second.at[s, z], sent.at[steps + s], got.at[steps + s], device(y, x, there, c))
    sums = []
    for s in range(steps):
        await_bytes(second.at[s, pl.ds(0, ZS - 1)], got.at[steps + s])
        sums.append(jnp.sum(second[s].astype(jnp.float32), axis=0).reshape(YS, -1, second.shape[-1]))
    total[...] = jnp.concatenate(sums, axis=1).astype(total.dtype)
    third[y] = total[y]
    for d in (2, 1, 3):
        there = (y + d) % YS
        send(total.at[there], third.at[y], sent.at[2 * steps], got.at[2 * steps], device(there, x, z, c))
    await_bytes(third.at[pl.ds(0, YS - 1)], got.at[2 * steps])
    columns = third.shape[-1]
    for e in range(YS):
        out[:, e * columns : (e + 1) * columns] = third[e]
    for s in range(steps):
        await_bytes(first.at[s, pl.ds(0, XS * CS - 1)], sent.at[s])
        await_bytes(second.at[s, pl.ds(0, ZS - 1)], sent.at[steps + s])
    await_bytes(third.at[pl.ds(0, YS - 1)], sent.at[2 * steps])


def give_back(outcome, mixing, row_count):
    steps, _, _, block, columns = outcome.shape
    vmem = pl.BlockSpec(memory_space=pltpu.VMEM)
    kept = outcome.dtype
    return pl.pallas_call(
        return_kernel,
        out_shape=jax.ShapeDtypeStruct((steps * row_count, YS * columns), kept),
        in_specs=[pl.BlockSpec(memory_space=pl.ANY), vmem],
        out_specs=vmem,
        scratch_shapes=[
            pltpu.VMEM((steps, CS * XS, YS, block, columns), kept),
            pltpu.VMEM((steps, ZS, YS * row_count, columns), kept),
            pltpu.VMEM((steps, ZS, YS * row_count, columns), kept),
            pltpu.VMEM((YS, steps * row_count, columns), kept),
            pltpu.VMEM((YS, steps * row_count, columns), kept),
            pltpu.SemaphoreType.DMA((2 * steps + 1,)),
            pltpu.SemaphoreType.DMA((2 * steps + 1,)),
            pltpu.SemaphoreType.DMA((steps,)),
        ],
        compiler_params=pltpu.CompilerParams(
            collective_id=1, has_side_effects=True, vmem_limit_bytes=48 * 1024 * 1024
        ),
        cost_estimate=pl.CostEstimate(flops=20_000_000_000, bytes_accessed=10_000_000, transcendentals=0),
        name="give_back",
    )(outcome, mixing)


def first_slots(named, capacity, axis):
    counted = named.astype(jnp.int32)
    before = jnp.cumsum(counted, axis=axis) - counted
    return jnp.stack([named & (before == slot) for slot in range(capacity)])


def layer(tokens, route_ids, route_weights, placement, expert_in, expert_down):
    experts = placement.shape[0]
    engines = lax.axis_size("engine")
    peers = lax.axis_size("ep")
    me = lax.axis_index("ep")
    _, _, my_z, _ = place()
    steps, row_count, width = tokens.shape
    capacity = 2
    tops = route_ids.shape[2]
    hidden_units = expert_in.shape[3]
    units = hidden_units // engines
    columns = width // engines
    numbers = jnp.arange(experts, dtype=jnp.int32)

    meta = jnp.concatenate([route_ids.astype(jnp.float32), route_weights], axis=2).reshape(steps * row_count, -1)
    meta = jnp.pad(meta, ((0, 0), (0, 128 - 2 * tops)))
    parts = jnp.concatenate([expert_in[..., e * units : (e + 1) * units] for e in range(engines)], axis=0)
    held_in = lax.all_to_all(parts, BOTH, split_axis=0, concat_axis=0, tiled=True)
    everyone, plane, cols = dispatch(tokens.reshape(steps * row_count, width), meta)

    named = jnp.any(plane[..., :tops] == me.astype(jnp.float32), axis=-1)
    named = named.reshape(peers, steps, row_count)
    slots = first_slots(named, capacity, 2)
    blocks = jnp.eye(peers, dtype=jnp.bool_)
    turns = jnp.eye(steps, dtype=jnp.bool_)
    slots = jnp.transpose(slots, (2, 1, 0, 3))
    chosen = slots[:, :, :, None, None, :] & blocks[None, :, None, :, None, None] & turns[:, None, None, None, :, None]
    chosen = chosen.reshape(steps * peers * capacity, peers * steps * row_count).astype(jnp.bfloat16)
    arrived = jnp.dot(chosen, everyone.reshape(-1, width), preferred_element_type=jnp.float32).astype(jnp.bfloat16)
    arrived = arrived.reshape(steps, peers * capacity, width)
    gathered = lax.all_gather(arrived, "engine", axis=1, tiled=True)

    near = jnp.arange(CS * XS, dtype=jnp.int32)
    near = (near % XS) * (ZS * CS) + my_z * CS + near // XS
    ids = cols[..., :tops].reshape(YS, ZS, steps, row_count, tops)
    wanted = ids[..., None] == near.astype(jnp.float32)
    strength = cols[..., tops : 2 * tops].reshape(YS, ZS, steps, row_count, tops)
    strength = jnp.sum(jnp.where(wanted, strength[..., None], 0.0), axis=4)
    filled = first_slots(jnp.any(wanted, axis=4), capacity, 3)
    shares = jnp.transpose(jnp.where(filled, strength[None], 0.0), (3, 2, 1, 4, 5, 0))
    same_y, same_z = jnp.eye(YS, dtype=jnp.bool_), jnp.eye(ZS, dtype=jnp.bool_)
    same = same_y[None, None, :, None, None, :, None, None] & same_z[None, :, None, None, None, None, :, None]
    mixing = jnp.where(same, shares[:, :, :, :, :, None, None, :], 0.0)
    mixing = mixing.reshape(steps, ZS * YS * row_count, CS * XS * YS * ZS * capacity)

    down = jnp.transpose(expert_down, (0, 2, 1))
    down_top = jnp.max(jnp.abs(down), axis=2).astype(jnp.float32)
    down_scale = (down_top + EPSILON) / quant_levels
    quant_down = jnp.floor(down.astype(jnp.float32) / down_scale[:, :, None] + 0.5).astype(jnp.bfloat16)
    held_down = lax.all_to_all(quant_down, "ep", split_axis=0, concat_axis=0, tiled=True)
    owners = jnp.sum(jnp.where(placement[None, :] == numbers[:, None], numbers[None, :], 0), axis=1)
    both_orders = jnp.stack([down_scale[owners], down_scale], axis=1)
    own_columns = (jnp.arange(peers) == me)[None, None, :, None]
    spread = jnp.where(own_columns, both_orders[:, :, None, :], 0.0).reshape(experts, 2, columns)
    both_scales = lax.psum_scatter(spread, "ep", scatter_dimension=0, tiled=True)
    out_scales, scale_out = both_scales[:, 0], both_scales[0, 1]

    top = jnp.max(jnp.abs(held_in), axis=(0, 2)).astype(jnp.float32)
    scale_in = (top + EPSILON) / quant_levels
    quant_in = jnp.floor(held_in.astype(jnp.float32) / scale_in[None, :, None, :] + 0.5).astype(jnp.bfloat16)
    quant_in = jnp.transpose(quant_in, (1, 0, 2, 3)).reshape(2, width, units)
    my_slot = jnp.sum(jnp.where(numbers == me, placement, 0))
    spread_in = jnp.where((numbers == my_slot)[:, None, None], scale_in[None], 0.0)
    projected = jnp.einsum("snd,mdf->msnf", gathered, quant_in, preferred_element_type=jnp.float32)
    projected = projected * scale_in[:, None, None, :]
    hidden = (jax.nn.silu(projected[0]) * projected[1]).astype(jnp.bfloat16)
    hidden = lax.all_gather(hidden, "engine", axis=0, tiled=False)
    spread_in, hidden, scale_out = lax.optimization_barrier((spread_in, hidden, scale_out))
    in_scales = lax.psum_scatter(spread_in, "ep", scatter_dimension=0, tiled=True)
    hidden = jnp.concatenate([hidden[e] for e in range(engines)], axis=-1)
    summed = jnp.einsum(
        "snf,cf->snc", hidden, held_down.reshape(-1, hidden_units), preferred_element_type=jnp.float32
    )
    outcome = (summed * scale_out).astype(jnp.bfloat16)
    outcome = outcome.reshape(steps, YS, CS * XS, ZS * capacity, columns)
    combined = give_back(outcome, mixing, row_count)
    return (combined.reshape(steps, row_count, width), in_scales, out_scales)


def solution(mesh):
    placed = (
        P(None, ("engine", "ep"), None),
        P(None, ("engine", "ep"), None),
        P(None, ("engine", "ep"), None),
        P(),
        P(None, None, ("engine", "ep"), None),
        P(None, None, ("engine", "ep")),
    )
    return jax.shard_map(
        layer,
        mesh=mesh,
        in_specs=placed,
        out_specs=(P(None, ("engine", "ep"), None), P("ep", None, "engine"), P("ep", "engine")),
        check_vma=False,
    )
```

```python
import jax
import jax.numpy as jnp
from jax import lax
from jax.experimental import pallas as pl
from jax.experimental.pallas import tpu as pltpu
from jax.sharding import PartitionSpec as P

EPSILON = 1e-06
quant_levels = 31.0
BOTH = ("engine", "ep")
MESH = pl.DeviceIdType.MESH
XS, ZS, CS, YS = 4, 8, 2, 4


def place():
    p = lax.axis_index("ep")
    return lax.axis_index("engine"), p // (ZS * CS), (p // CS) % ZS, p % CS


def device(y, x, z, c):
    return {"engine": y, "ep": x * (ZS * CS) + z * CS + c}


def peers_of(kind):
    y, x, z, c = place()
    if kind == "z":
        return [device(y, x, (z + d) % ZS, c) for d in (4, 3, 5, 2, 6, 1, 7)]
    if kind == "x":
        return [device(y, (x + d) % XS, z, c) for d in (2, 1, 3)]
    if kind == "y":
        return [device((y + d) % YS, x, z, c) for d in (2, 1, 3)]
    if kind == "c":
        return [device(y, x, z, 1 - c)]
    return [device(y, (x + d) % XS, z, (c + f) % CS) for f in (0, 1) for d in range(XS) if (d, f) != (0, 0)]


def greet(kinds):
    barrier = pltpu.get_barrier_semaphore()
    count = 0
    for kind in kinds:
        for peer in peers_of(kind):
            pl.semaphore_signal(barrier, inc=1, device_id=peer, device_id_type=MESH)
            count += 1
    pl.semaphore_wait(barrier, count)


def send(src, dst, send_sem, recv_sem, peer):
    copy = pltpu.make_async_remote_copy(
        src_ref=src, dst_ref=dst, send_sem=send_sem, recv_sem=recv_sem, device_id=peer, device_id_type=MESH
    )
    copy.start()
    return copy


def await_bytes(like, sem):
    pltpu.make_async_copy(like, like, sem).wait()


def notes_kernel(meta_ref, plane, cols, sent, got):
    y, x, z, c = place()
    greet(("z", "x", "y", "c"))
    for peer in peers_of("z"):
        send(meta_ref, plane.at[c, x, z], sent.at[0], got.at[0], peer)
    plane[c, x, z] = meta_ref[...]
    await_bytes(plane.at[c, x, pl.ds(0, ZS - 1)], got.at[0])
    for peer in peers_of("x"):
        send(plane.at[c, x], plane.at[c, x], sent.at[1], got.at[1], peer)
    for peer in peers_of("y"):
        send(plane.at[c, x], cols.at[y], sent.at[2], got.at[2], peer)
    cols[y] = plane[c, x]
    await_bytes(plane.at[c, pl.ds(0, XS - 1)], got.at[1])
    for peer in peers_of("c"):
        send(plane.at[c], plane.at[c], sent.at[3], got.at[3], peer)
    await_bytes(cols.at[pl.ds(0, YS - 1)], got.at[2])
    await_bytes(plane.at[c], got.at[3])
    await_bytes(plane.at[c, x, pl.ds(0, ZS - 1)], sent.at[0])
    await_bytes(plane.at[c, pl.ds(0, XS - 1)], sent.at[1])
    await_bytes(cols.at[pl.ds(0, YS - 1)], sent.at[2])
    await_bytes(plane.at[c], sent.at[3])


def pass_notes(meta):
    vmem = pl.BlockSpec(memory_space=pltpu.VMEM)
    return pl.pallas_call(
        notes_kernel,
        out_shape=(
            jax.ShapeDtypeStruct((CS, XS, ZS) + meta.shape, meta.dtype),
            jax.ShapeDtypeStruct((YS, ZS) + meta.shape, meta.dtype),
        ),
        in_specs=[vmem],
        out_specs=(vmem, vmem),
        scratch_shapes=[pltpu.SemaphoreType.DMA((4,)), pltpu.SemaphoreType.DMA((4,))],
        compiler_params=pltpu.CompilerParams(collective_id=0, has_side_effects=True),
        name="notes",
    )(meta)


def return_kernel(outcome, mixing, scales, out, heard, first, partial, second, total, third, sent, got, own):
    steps = outcome.shape[0]
    y, x, z, c = place()
    here = c * XS + x
    greet(("xc", "z", "y"))
    locals_ = []
    last = 2 * steps + 1
    heard[here, z] = scales[...]
    for f, d in ((0, 2), (0, 1), (0, 3), (1, 2), (1, 1), (1, 3), (1, 0)):
        peer = device(y, (x + d) % XS, z, (c + f) % CS)
        send(scales, heard.at[here, z], sent.at[last], got.at[last], peer)
    for s in range(steps):
        local = pltpu.make_async_copy(outcome.at[s, :, here], first.at[s, here], own.at[s])
        local.start()
        locals_.append(local)
        for f, d in ((0, 2), (0, 1), (0, 3), (1, 2), (1, 1), (1, 3), (1, 0)):
            there_x, there_c = (x + d) % XS, (c + f) % CS
            src = outcome.at[s, :, there_c * XS + there_x]
            send(src, first.at[s, here], sent.at[s], got.at[s], device(y, there_x, z, there_c))
    for s in range(steps):
        locals_[s].wait()
        await_bytes(first.at[s, pl.ds(0, XS * CS - 1)], got.at[s])
        rows = first[s].reshape(-1, first.shape[-1]).astype(jnp.float32)
        sums = jnp.dot(mixing[s], rows, precision=lax.Precision.HIGHEST, preferred_element_type=jnp.float32)
        partial[s] = sums.astype(partial.dtype).reshape(partial.shape[1:])
        second[s, z] = partial[s, z]
        for d in (4, 3, 5, 2, 6, 1, 7):
            there = (z + d) % ZS
            send(partial.at[s, there], second.at[s, z], sent.at[steps + s], got.at[steps + s], device(y, x, there, c))
    await_bytes(heard.at[pl.ds(0, XS * CS - 1), z], got.at[last])
    for peer in peers_of("z"):
        send(heard.at[:, z], heard.at[:, z], sent.at[last + 1], got.at[last + 1], peer)
    sums = []
    for s in range(steps):
        await_bytes(second.at[s, pl.ds(0, ZS - 1)], got.at[steps + s])
        sums.append(jnp.sum(second[s].astype(jnp.float32), axis=0).reshape(YS, -1, second.shape[-1]))
    total[...] = jnp.concatenate(sums, axis=1).astype(total.dtype)
    third[y] = total[y]
    for d in (2, 1, 3):
        there = (y + d) % YS
        send(total.at[there], third.at[y], sent.at[2 * steps], got.at[2 * steps], device(there, x, z, c))
    await_bytes(third.at[pl.ds(0, YS - 1)], got.at[2 * steps])
    columns = third.shape[-1]
    for e in range(YS):
        out[:, e * columns : (e + 1) * columns] = third[e]
    await_bytes(heard.at[:, pl.ds(0, ZS - 1)], got.at[last + 1])
    await_bytes(heard.at[pl.ds(0, XS * CS - 1), z], sent.at[last])
    await_bytes(heard.at[:, pl.ds(0, ZS - 1)], sent.at[last + 1])
    for s in range(steps):
        await_bytes(first.at[s, pl.ds(0, XS * CS - 1)], sent.at[s])
        await_bytes(second.at[s, pl.ds(0, ZS - 1)], sent.at[steps + s])
    await_bytes(third.at[pl.ds(0, YS - 1)], sent.at[2 * steps])


def give_back(outcome, mixing, scales, row_count):
    steps, _, _, block, columns = outcome.shape
    vmem = pl.BlockSpec(memory_space=pltpu.VMEM)
    kept = outcome.dtype
    return pl.pallas_call(
        return_kernel,
        out_shape=(
            jax.ShapeDtypeStruct((steps * row_count, YS * columns), kept),
            jax.ShapeDtypeStruct((XS * CS, ZS) + scales.shape, scales.dtype),
        ),
        in_specs=[pl.BlockSpec(memory_space=pl.ANY), vmem, vmem],
        out_specs=(vmem, vmem),
        scratch_shapes=[
            pltpu.VMEM((steps, CS * XS, YS, block, columns), kept),
            pltpu.VMEM((steps, ZS, YS * row_count, columns), kept),
            pltpu.VMEM((steps, ZS, YS * row_count, columns), kept),
            pltpu.VMEM((YS, steps * row_count, columns), kept),
            pltpu.VMEM((YS, steps * row_count, columns), kept),
            pltpu.SemaphoreType.DMA((2 * steps + 3,)),
            pltpu.SemaphoreType.DMA((2 * steps + 3,)),
            pltpu.SemaphoreType.DMA((steps,)),
        ],
        compiler_params=pltpu.CompilerParams(
            collective_id=1, has_side_effects=True, vmem_limit_bytes=48 * 1024 * 1024
        ),
        cost_estimate=pl.CostEstimate(flops=20_000_000_000, bytes_accessed=10_000_000, transcendentals=0),
        name="give_back",
    )(outcome, mixing, scales)


def slot_codes(named, base, axis):
    counted = named.astype(jnp.int32)
    return jnp.where(named, base + jnp.cumsum(counted, axis=axis) - counted, -1)


def layer(tokens, route_ids, route_weights, placement, expert_in, expert_down):
    experts = placement.shape[0]
    engines = lax.axis_size("engine")
    peers = lax.axis_size("ep")
    me = lax.axis_index("ep")
    _, _, my_z, _ = place()
    steps, row_count, width = tokens.shape
    capacity = 2
    tops = route_ids.shape[2]
    hidden_units = expert_in.shape[3]
    units = hidden_units // engines
    columns = width // engines
    numbers = jnp.arange(experts, dtype=jnp.int32)

    everyone = lax.all_gather(tokens, "ep", axis=0, tiled=False)
    meta = jnp.concatenate([route_ids.astype(jnp.float32), route_weights], axis=2).reshape(steps * row_count, -1)
    meta = jnp.pad(meta, ((0, 0), (0, 128 - 2 * tops)))
    plane, cols = pass_notes(meta)
    parts = jnp.concatenate([expert_in[..., e * units : (e + 1) * units] for e in range(engines)], axis=0)
    parts, plane = lax.optimization_barrier((parts, plane))
    held_in = lax.all_to_all(parts, BOTH, split_axis=0, concat_axis=0, tiled=True)
    held_down = lax.all_to_all(
        jnp.transpose(expert_down, (0, 2, 1)), "ep", split_axis=0, concat_axis=0, tiled=True
    ).reshape(columns, hidden_units)

    named = jnp.any(plane[..., :tops] == me.astype(jnp.float32), axis=-1)
    named = jnp.transpose(named, (1, 2, 0, 3)).reshape(XS, ZS, CS, steps, row_count)
    at_x = jnp.arange(XS, dtype=jnp.int32)[:, None, None, None, None]
    at_z = jnp.arange(ZS, dtype=jnp.int32)[None, :, None, None, None]
    at_c = jnp.arange(CS, dtype=jnp.int32)[None, None, :, None, None]
    codes = slot_codes(named, ((at_c * XS + at_x) * ZS + at_z) * capacity, 4)
    codes = jnp.transpose(codes, (3, 0, 1, 2, 4)).reshape(steps, peers * row_count)
    slots = jnp.arange(peers * capacity, dtype=jnp.int32)
    arrived = []
    for step in range(steps):
        chosen = (slots[:, None] == codes[step][None, :]).astype(jnp.bfloat16)
        rows = everyone[:, step].reshape(peers * row_count, width)
        arrived.append(jnp.dot(chosen, rows, preferred_element_type=jnp.float32).astype(jnp.bfloat16))
    arrived = jnp.stack(arrived)
    gathered = lax.all_gather(arrived, "engine", axis=1, tiled=True)

    near = jnp.arange(CS * XS, dtype=jnp.int32)
    expert_of = (near % XS) * (ZS * CS) + my_z * CS + near // XS
    ids = jnp.transpose(cols[..., :tops].reshape(YS, ZS, steps, row_count, tops), (2, 1, 0, 3, 4))
    strength = jnp.transpose(cols[..., tops : 2 * tops].reshape(YS, ZS, steps, row_count, tops), (2, 1, 0, 3, 4))
    wanted = ids[..., None] == expert_of.astype(jnp.float32)
    strength = jnp.sum(jnp.where(wanted, strength[..., None], 0.0), axis=4)
    base = near * (YS * ZS) + jnp.arange(YS, dtype=jnp.int32)[None, None, :, None, None] * ZS
    base = (base + jnp.arange(ZS, dtype=jnp.int32)[None, :, None, None, None]) * capacity
    spots = slot_codes(jnp.any(wanted, axis=4), base, 3)
    lanes = jnp.arange(CS * XS * YS * ZS * capacity, dtype=jnp.int32)
    spots = spots.reshape(steps, ZS * YS * row_count, CS * XS)
    strength = strength.reshape(steps, ZS * YS * row_count, CS * XS)
    mixing = sum(
        jnp.where(spots[:, :, n, None] == lanes, strength[:, :, n, None], 0.0) for n in range(CS * XS)
    )

    top = jnp.max(jnp.abs(held_in), axis=(0, 2)).astype(jnp.float32)
    scale_in = (top + EPSILON) / quant_levels
    quant_in = jnp.floor(held_in.astype(jnp.float32) / scale_in[None, :, None, :] + 0.5).astype(jnp.bfloat16)
    quant_in = jnp.transpose(quant_in, (1, 0, 2, 3)).reshape(2, width, units)
    projected = jnp.einsum("snd,mdf->msnf", gathered, quant_in, preferred_element_type=jnp.float32)
    projected = projected * scale_in[:, None, None, :]
    hidden = (jax.nn.silu(projected[0]) * projected[1]).astype(jnp.bfloat16)
    hidden = lax.all_gather(hidden, "engine", axis=0, tiled=False)
    hidden = jnp.concatenate([hidden[e] for e in range(engines)], axis=-1)

    scale_out = (jnp.max(jnp.abs(held_down), axis=1).astype(jnp.float32) + EPSILON) / quant_levels
    quant_down = jnp.floor(held_down.astype(jnp.float32) / scale_out[:, None] + 0.5).astype(jnp.bfloat16)
    summed = jnp.einsum("snf,cf->snc", hidden, quant_down, preferred_element_type=jnp.float32)
    outcome = (summed * scale_out).astype(jnp.bfloat16)
    outcome = outcome.reshape(steps, YS, CS * XS, ZS * capacity, columns)
    scales = jnp.concatenate([scale_in.reshape(-1), scale_out, jnp.zeros((256,), jnp.float32)]).reshape(16, 128)
    combined, heard = give_back(outcome, mixing, scales, row_count)
    mine = jnp.sum(jnp.where(placement == me, numbers, 0))
    spot = ((mine % CS) * XS + mine // (ZS * CS)) * ZS + (mine // CS) % ZS
    picked = lax.dynamic_index_in_dim(heard.reshape(experts, -1), spot, 0, keepdims=False)
    in_scales = picked[: 2 * units].reshape(1, 2, units)
    out_scales = picked[2 * units : 2 * units + columns].reshape(1, columns)
    return (combined.reshape(steps, row_count, width), in_scales, out_scales)


def solution(mesh):
    placed = (
        P(None, ("engine", "ep"), None),
        P(None, ("engine", "ep"), None),
        P(None, ("engine", "ep"), None),
        P(),
        P(None, None, ("engine", "ep"), None),
        P(None, None, ("engine", "ep")),
    )
    return jax.shard_map(
        layer,
        mesh=mesh,
        in_specs=placed,
        out_specs=(P(None, ("engine", "ep"), None), P("ep", None, "engine"), P("ep", "engine")),
        check_vma=False,
    )
```

```python
import jax
import jax.numpy as jnp
from jax import lax
from jax.experimental import pallas as pl
from jax.experimental.pallas import tpu as pltpu
from jax.sharding import PartitionSpec as P


EPSILON = 1e-06
quant_levels = 31.0
BOTH = ("engine", "ep")
MESH = pl.DeviceIdType.MESH
XS, ZS, CS, YS = 4, 8, 2, 4


def place():
    p = lax.axis_index("ep")
    return lax.axis_index("engine"), p // (ZS * CS), (p // CS) % ZS, p % CS


def device(y, x, z, c):
    return {"engine": y, "ep": x * (ZS * CS) + z * CS + c}


def peers_of(kind):
    y, x, z, c = place()
    if kind == "z":
        return [device(y, x, (z + d) % ZS, c) for d in (4, 3, 5, 2, 6, 1, 7)]
    if kind == "x":
        return [device(y, (x + d) % XS, z, c) for d in (2, 1, 3)]
    if kind == "y":
        return [device((y + d) % YS, x, z, c) for d in (2, 1, 3)]
    if kind == "c":
        return [device(y, x, z, 1 - c)]
    return [device(y, (x + d) % XS, z, (c + f) % CS) for f in (0, 1) for d in range(XS) if (d, f) != (0, 0)]


def greet(kinds):
    barrier = pltpu.get_barrier_semaphore()
    count = 0
    for kind in kinds:
        for peer in peers_of(kind):
            pl.semaphore_signal(barrier, inc=1, device_id=peer, device_id_type=MESH)
            count += 1
    pl.semaphore_wait(barrier, count)


def send(src, dst, send_sem, recv_sem, peer):
    copy = pltpu.make_async_remote_copy(
        src_ref=src, dst_ref=dst, send_sem=send_sem, recv_sem=recv_sem, device_id=peer, device_id_type=MESH
    )
    copy.start()
    return copy


def await_bytes(like, sem):
    pltpu.make_async_copy(like, like, sem).wait()


def return_kernel(outcome, mixing, scales, out, heard, first, partial, second, total, third, sent, got, own):
    steps, block = mixing.shape[0], first.shape[3]
    y, x, z, c = place()
    here = c * XS + x

    def rows_for(s, peer):
        return outcome.at[:, pl.ds(pl.multiple_of((s * CS * XS + peer) * block, block), block)]

    greet(("xc", "z", "y"))
    locals_ = []
    last = 2 * steps + 1
    heard[here, z] = scales[...]
    for f, d in ((0, 2), (0, 1), (0, 3), (1, 2), (1, 1), (1, 3), (1, 0)):
        peer = device(y, (x + d) % XS, z, (c + f) % CS)
        send(scales, heard.at[here, z], sent.at[last], got.at[last], peer)
    for s in range(steps):
        local = pltpu.make_async_copy(rows_for(s, here), first.at[s, here], own.at[s])
        local.start()
        locals_.append(local)
        for f, d in ((0, 2), (0, 1), (0, 3), (1, 2), (1, 1), (1, 3), (1, 0)):
            there_x, there_c = (x + d) % XS, (c + f) % CS
            src = rows_for(s, there_c * XS + there_x)
            send(src, first.at[s, here], sent.at[s], got.at[s], device(y, there_x, z, there_c))
    for s in range(steps):
        locals_[s].wait()
        await_bytes(first.at[s, pl.ds(0, XS * CS - 1)], got.at[s])
        rows = first[s].reshape(-1, first.shape[-1]).astype(jnp.float32)
        sums = jnp.dot(mixing[s], rows, precision=lax.Precision.HIGHEST, preferred_element_type=jnp.float32)
        partial[s] = sums.astype(partial.dtype).reshape(partial.shape[1:])
        second[s, z] = partial[s, z]
        for d in (4, 3, 5, 2, 6, 1, 7):
            there = (z + d) % ZS
            send(partial.at[s, there], second.at[s, z], sent.at[steps + s], got.at[steps + s], device(y, x, there, c))
    await_bytes(heard.at[pl.ds(0, XS * CS - 1), z], got.at[last])
    for peer in peers_of("z"):
        send(heard.at[:, z], heard.at[:, z], sent.at[last + 1], got.at[last + 1], peer)
    sums = []
    for s in range(steps):
        await_bytes(second.at[s, pl.ds(0, ZS - 1)], got.at[steps + s])
        sums.append(jnp.sum(second[s].astype(jnp.float32), axis=0).reshape(YS, -1, second.shape[-1]))
    total[...] = jnp.concatenate(sums, axis=1).astype(total.dtype)
    third[y] = total[y]
    for d in (2, 1, 3):
        there = (y + d) % YS
        send(total.at[there], third.at[y], sent.at[2 * steps], got.at[2 * steps], device(there, x, z, c))
    await_bytes(third.at[pl.ds(0, YS - 1)], got.at[2 * steps])
    columns = third.shape[-1]
    for e in range(YS):
        out[:, e * columns : (e + 1) * columns] = third[e]
    await_bytes(heard.at[:, pl.ds(0, ZS - 1)], got.at[last + 1])
    await_bytes(heard.at[pl.ds(0, XS * CS - 1), z], sent.at[last])
    await_bytes(heard.at[:, pl.ds(0, ZS - 1)], sent.at[last + 1])
    for s in range(steps):
        await_bytes(first.at[s, pl.ds(0, XS * CS - 1)], sent.at[s])
        await_bytes(second.at[s, pl.ds(0, ZS - 1)], sent.at[steps + s])
    await_bytes(third.at[pl.ds(0, YS - 1)], sent.at[2 * steps])


def give_back(outcome, mixing, scales, row_count, block):
    steps, columns = mixing.shape[0], outcome.shape[-1]
    vmem = pl.BlockSpec(memory_space=pltpu.VMEM)
    kept = outcome.dtype
    return pl.pallas_call(
        return_kernel,
        out_shape=(
            jax.ShapeDtypeStruct((steps * row_count, YS * columns), kept),
            jax.ShapeDtypeStruct((XS * CS, ZS) + scales.shape, scales.dtype),
        ),
        in_specs=[pl.BlockSpec(memory_space=pl.ANY), vmem, vmem],
        out_specs=(vmem, vmem),
        scratch_shapes=[
            pltpu.VMEM((steps, CS * XS, YS, block, columns), kept),
            pltpu.VMEM((steps, ZS, YS * row_count, columns), kept),
            pltpu.VMEM((steps, ZS, YS * row_count, columns), kept),
            pltpu.VMEM((YS, steps * row_count, columns), kept),
            pltpu.VMEM((YS, steps * row_count, columns), kept),
            pltpu.SemaphoreType.DMA((2 * steps + 3,)),
            pltpu.SemaphoreType.DMA((2 * steps + 3,)),
            pltpu.SemaphoreType.DMA((steps,)),
        ],
        compiler_params=pltpu.CompilerParams(
            collective_id=0, has_side_effects=True, vmem_limit_bytes=48 * 1024 * 1024
        ),
        cost_estimate=pl.CostEstimate(flops=20_000_000_000, bytes_accessed=10_000_000, transcendentals=0),
        name="give_back",
    )(outcome, mixing, scales)


def exact_parts(values):
    high = lax.reduce_precision(values, 8, 7)
    middle = lax.reduce_precision(values - high, 8, 7)
    return [part.astype(jnp.bfloat16) for part in (high, middle, values - high - middle)]


def layer(tokens, route_ids, route_weights, placement, expert_in, expert_down):
    experts = placement.shape[0]
    engines = lax.axis_size("engine")
    peers = lax.axis_size("ep")
    me = lax.axis_index("ep")
    _, _, my_z, _ = place()
    steps, row_count, width = tokens.shape
    capacity = 2
    tops = route_ids.shape[2]
    hidden_units = expert_in.shape[3]
    units = hidden_units // engines
    columns = width // engines
    numbers = jnp.arange(experts, dtype=jnp.int32)
    z_groups = [[x * ZS * CS + z * CS + c for z in range(ZS)] for x in range(XS) for c in range(CS)]
    xc_groups = [[x * ZS * CS + z * CS + c for c in range(CS) for x in range(XS)] for z in range(ZS)]

    same = route_ids[:, :, None, :, None] == route_ids[:, None, :, None, :]
    earlier = jnp.arange(row_count)[:, None] > jnp.arange(row_count)[None, :]
    before = jnp.sum((same & earlier[None, :, :, None, None]).astype(jnp.int32), axis=(2, 4))
    marks = (route_ids * capacity + before).astype(jnp.bfloat16)
    notes = jnp.concatenate([marks] + exact_parts(route_weights), axis=2)
    notes = jnp.pad(notes, ((0, 0), (0, 0), (0, 128 - 4 * tops)))
    payload = jnp.concatenate([tokens, notes], axis=2).reshape(steps * row_count, -1)
    column = lax.all_gather(payload, "ep", axis_index_groups=z_groups, axis=0, tiled=False)
    everyone = lax.all_gather(column, "ep", axis_index_groups=xc_groups, axis=0, tiled=False)
    parts = jnp.concatenate([expert_in[..., e * units : (e + 1) * units] for e in range(engines)], axis=0)
    held_in = lax.all_to_all(parts, BOTH, split_axis=0, concat_axis=0, tiled=True)
    held_down = lax.all_to_all(
        jnp.transpose(expert_down, (0, 2, 1)), "ep", split_axis=0, concat_axis=0, tiled=True
    )
    held_down = held_down.reshape(columns, hidden_units)

    marks = everyone[..., width : width + tops].reshape(peers, steps, row_count, tops)
    first = (me * capacity).astype(jnp.bfloat16)
    slot = jnp.where(jnp.any(marks == first, axis=3), 0, jnp.where(jnp.any(marks == first + 1, axis=3), 1, -1))
    base = jnp.arange(peers, dtype=jnp.int32)[:, None, None] * capacity
    base = base + jnp.arange(steps, dtype=jnp.int32)[None, :, None] * (peers * capacity)
    codes = jnp.where(slot >= 0, base + slot, -1).reshape(-1)
    slots = jnp.arange(steps * peers * capacity, dtype=jnp.int32)
    chosen = (slots[:, None] == codes[None, :]).astype(jnp.bfloat16)
    arrived = jnp.dot(
        chosen, everyone.reshape(-1, everyone.shape[-1]), preferred_element_type=jnp.float32
    ).astype(jnp.bfloat16)[:, :width]
    notes = column[..., width : width + 4 * tops].reshape(-1, width)
    notes = jnp.pad(notes, ((0, 8 - notes.shape[0]), (0, 0)))
    gathered = lax.all_gather(jnp.concatenate([arrived, notes]), "engine", axis=0, tiled=False)
    row_total = arrived.shape[0]

    notes = gathered[:, row_total].reshape(YS, ZS, steps, row_count, 4 * tops)
    notes = jnp.transpose(notes, (2, 1, 0, 3, 4)).reshape(steps, ZS * YS * row_count, 4, tops).astype(jnp.float32)
    marks, strength = notes[:, :, 0], notes[:, :, 1] + notes[:, :, 2] + notes[:, :, 3]
    block = jnp.arange(ZS * YS * row_count, dtype=jnp.int32) // row_count
    block = ((block % YS) * ZS + block // YS) * capacity
    lanes = jnp.arange(CS * XS * YS * ZS * capacity, dtype=jnp.int32)
    near = jnp.arange(CS * XS, dtype=jnp.int32)
    target = (((near % XS) * (ZS * CS) + my_z * CS + near // XS) * capacity).astype(jnp.float32)
    lower = marks[..., None] == target
    upper = marks[..., None] == target + 1.0
    share = jnp.sum(jnp.where(lower | upper, strength[..., None], 0.0), axis=2)
    spot = block[:, None] + near * (YS * ZS * capacity) + jnp.any(upper, axis=2).astype(jnp.int32)
    mixing = sum(jnp.where(spot[:, :, n, None] == lanes, share[:, :, n, None], 0.0) for n in range(CS * XS))

    top = jnp.max(jnp.abs(held_in), axis=(0, 2)).astype(jnp.float32)
    scale_in = (top + EPSILON) / quant_levels
    quant_in = jnp.floor(held_in.astype(jnp.float32) / scale_in[None, :, None, :] + 0.5).astype(jnp.bfloat16)
    quant_in = jnp.transpose(quant_in, (1, 0, 2, 3)).reshape(2, width, units)
    rows = gathered.reshape(-1, width)
    projected = jnp.einsum("nd,mdf->mnf", rows, quant_in, preferred_element_type=jnp.float32)
    projected = projected * scale_in[:, None, :]
    hidden = (jax.nn.silu(projected[0]) * projected[1]).astype(jnp.bfloat16)
    hidden = lax.all_gather(hidden, "engine", axis=0, tiled=False)
    hidden = jnp.concatenate([hidden[e] for e in range(engines)], axis=-1)

    scale_out = (jnp.max(jnp.abs(held_down), axis=1).astype(jnp.float32) + EPSILON) / quant_levels
    quant_down = jnp.floor(held_down.astype(jnp.float32) / scale_out[:, None] + 0.5).astype(jnp.bfloat16)
    summed = jnp.einsum("nf,cf->nc", hidden, quant_down, preferred_element_type=jnp.float32)
    outcome = (summed * scale_out).astype(jnp.bfloat16)
    outcome = outcome.reshape(YS, -1, columns)
    scales = jnp.concatenate([scale_in.reshape(-1), scale_out, jnp.zeros((256,), jnp.float32)]).reshape(16, 128)
    combined, heard = give_back(outcome, mixing, scales, row_count, ZS * capacity)
    mine = jnp.sum(jnp.where(placement == me, numbers, 0))
    spot = ((mine % CS) * XS + mine // (ZS * CS)) * ZS + (mine // CS) % ZS
    picked = lax.dynamic_index_in_dim(heard.reshape(experts, -1), spot, 0, keepdims=False)
    in_scales = picked[: 2 * units].reshape(1, 2, units)
    out_scales = picked[2 * units : 2 * units + columns].reshape(1, columns)
    return (combined.reshape(steps, row_count, width), in_scales, out_scales)


def solution(mesh):
    placed = (
        P(None, ("engine", "ep"), None),
        P(None, ("engine", "ep"), None),
        P(None, ("engine", "ep"), None),
        P(),
        P(None, None, ("engine", "ep"), None),
        P(None, None, ("engine", "ep")),
    )
    return jax.shard_map(
        layer,
        mesh=mesh,
        in_specs=placed,
        out_specs=(P(None, ("engine", "ep"), None), P("ep", None, "engine"), P("ep", "engine")),
        check_vma=False,
    )
```

```python
import jax
import jax.numpy as jnp
from jax import lax
from jax.experimental import pallas as pl
from jax.experimental.pallas import tpu as pltpu
from jax.sharding import PartitionSpec as P


EPSILON = 1e-06
quant_levels = 31.0
BOTH = ("engine", "ep")
MESH = pl.DeviceIdType.MESH
XS, ZS, CS, YS = 4, 8, 2, 4


def place():
    p = lax.axis_index("ep")
    return lax.axis_index("engine"), p // (ZS * CS), (p // CS) % ZS, p % CS


def device(y, x, z, c):
    return {"engine": y, "ep": x * (ZS * CS) + z * CS + c}


def peers_of(kind):
    y, x, z, c = place()
    if kind == "z":
        return [device(y, x, (z + d) % ZS, c) for d in (4, 3, 5, 2, 6, 1, 7)]
    if kind == "x":
        return [device(y, (x + d) % XS, z, c) for d in (2, 1, 3)]
    if kind == "y":
        return [device((y + d) % YS, x, z, c) for d in (2, 1, 3)]
    if kind == "c":
        return [device(y, x, z, 1 - c)]
    return [device(y, (x + d) % XS, z, (c + f) % CS) for f in (0, 1) for d in range(XS) if (d, f) != (0, 0)]


def greet(kinds):
    barrier = pltpu.get_barrier_semaphore()
    count = 0
    for kind in kinds:
        for peer in peers_of(kind):
            pl.semaphore_signal(barrier, inc=1, device_id=peer, device_id_type=MESH)
            count += 1
    pl.semaphore_wait(barrier, count)


def send(src, dst, send_sem, recv_sem, peer):
    copy = pltpu.make_async_remote_copy(
        src_ref=src, dst_ref=dst, send_sem=send_sem, recv_sem=recv_sem, device_id=peer, device_id_type=MESH
    )
    copy.start()
    return copy


def await_bytes(like, sem):
    pltpu.make_async_copy(like, like, sem).wait()


def return_kernel(outcome, mixing, scales, out, heard, first, partial, second, total, third, sent, got, own):
    steps, halves, block, part = mixing.shape[0], first.shape[0], first.shape[4], first.shape[5]
    y, x, z, c = place()
    here = c * XS + x
    note = 2 * steps * halves
    chunks = [(h, s) for h in range(halves) for s in range(steps)]

    def rows_for(h, s, peer):
        return outcome.at[s, :, pl.ds(pl.multiple_of(peer * block, block), block), pl.ds(h * part, part)]

    greet(("xc", "z", "y"))
    heard[here, z] = scales[...]
    own_copies = []
    for k, (h, s) in enumerate(chunks):
        own_copies.append(pltpu.make_async_copy(rows_for(h, s, here), first.at[h, s, here], own.at[k]))
        own_copies[k].start()
        for f, d in ((0, 2), (1, 2), (0, 1), (0, 3), (1, 1), (1, 3), (1, 0)):
            there_x, there_c = (x + d) % XS, (c + f) % CS
            src = rows_for(h, s, there_c * XS + there_x)
            send(src, first.at[h, s, here], sent.at[k], got.at[k], device(y, there_x, z, there_c))
        if k == 0:
            for f, d in ((0, 2), (0, 1), (0, 3), (1, 2), (1, 1), (1, 3), (1, 0)):
                peer = device(y, (x + d) % XS, z, (c + f) % CS)
                send(scales, heard.at[here, z], sent.at[note], got.at[note], peer)
    for k, (h, s) in enumerate(chunks):
        own_copies[k].wait()
        await_bytes(first.at[h, s, pl.ds(0, XS * CS - 1)], got.at[k])
        rows = first[h, s].reshape(-1, part).astype(jnp.float32)
        sums = jnp.dot(mixing[s], rows, precision=lax.Precision.HIGHEST, preferred_element_type=jnp.float32)
        partial[h, s] = sums.astype(partial.dtype).reshape(partial.shape[2:])
        second[h, s, z] = partial[h, s, z]
        for d in (4, 3, 5, 2, 6, 1, 7):
            there = (z + d) % ZS
            pair = note + 3 + k
            send(partial.at[h, s, there], second.at[h, s, z], sent.at[pair], got.at[pair], device(y, x, there, c))
        if k == 0:
            await_bytes(heard.at[pl.ds(0, XS * CS - 1), z], got.at[note])
            for peer in peers_of("z"):
                send(heard.at[:, z], heard.at[:, z], sent.at[note + 1], got.at[note + 1], peer)
    for h in range(halves):
        sums = []
        for s in range(steps):
            await_bytes(second.at[h, s, pl.ds(0, ZS - 1)], got.at[note + 3 + h * steps + s])
            sums.append(jnp.sum(second[h, s].astype(jnp.float32), axis=0).reshape(YS, -1, part))
        total[h] = jnp.concatenate(sums, axis=1).astype(total.dtype)
        third[h, y] = total[h, y]
        for d in (2, 1, 3):
            there = (y + d) % YS
            last = steps * halves + h
            send(total.at[h, there], third.at[h, y], sent.at[last], got.at[last], device(there, x, z, c))
    for h in range(halves):
        await_bytes(third.at[h, pl.ds(0, YS - 1)], got.at[steps * halves + h])
        for e in range(YS):
            start = (e * halves + h) * part
            out[:, start : start + part] = third[h, e]
    await_bytes(heard.at[:, pl.ds(0, ZS - 1)], got.at[note + 1])
    await_bytes(heard.at[pl.ds(0, XS * CS - 1), z], sent.at[note])
    await_bytes(heard.at[:, pl.ds(0, ZS - 1)], sent.at[note + 1])
    for k, (h, s) in enumerate(chunks):
        await_bytes(first.at[h, s, pl.ds(0, XS * CS - 1)], sent.at[k])
        await_bytes(second.at[h, s, pl.ds(0, ZS - 1)], sent.at[note + 3 + k])
    for h in range(halves):
        await_bytes(third.at[h, pl.ds(0, YS - 1)], sent.at[steps * halves + h])


def give_back(outcome, mixing, scales, row_count, block, halves=2):
    steps, columns = mixing.shape[0], outcome.shape[-1]
    part = columns // halves
    vmem = pl.BlockSpec(memory_space=pltpu.VMEM)
    kept = outcome.dtype
    count = 3 * steps * halves + 3
    return pl.pallas_call(
        return_kernel,
        out_shape=(
            jax.ShapeDtypeStruct((steps * row_count, YS * columns), kept),
            jax.ShapeDtypeStruct((XS * CS, ZS) + scales.shape, scales.dtype),
        ),
        in_specs=[pl.BlockSpec(memory_space=pl.ANY), vmem, vmem],
        out_specs=(vmem, vmem),
        scratch_shapes=[
            pltpu.VMEM((halves, steps, CS * XS, YS, block, part), kept),
            pltpu.VMEM((halves, steps, ZS, YS * row_count, part), kept),
            pltpu.VMEM((halves, steps, ZS, YS * row_count, part), kept),
            pltpu.VMEM((halves, YS, steps * row_count, part), kept),
            pltpu.VMEM((halves, YS, steps * row_count, part), kept),
            pltpu.SemaphoreType.DMA((count,)),
            pltpu.SemaphoreType.DMA((count,)),
            pltpu.SemaphoreType.DMA((steps * halves,)),
        ],
        compiler_params=pltpu.CompilerParams(
            collective_id=0, has_side_effects=True, vmem_limit_bytes=48 * 1024 * 1024
        ),
        cost_estimate=pl.CostEstimate(flops=20_000_000_000, bytes_accessed=10_000_000, transcendentals=0),
        name="give_back",
    )(outcome, mixing, scales)


def exact_parts(values):
    high = lax.reduce_precision(values, 8, 7)
    middle = lax.reduce_precision(values - high, 8, 7)
    return [part.astype(jnp.bfloat16) for part in (high, middle, values - high - middle)]


def layer(tokens, route_ids, route_weights, placement, expert_in, expert_down):
    experts = placement.shape[0]
    engines = lax.axis_size("engine")
    peers = lax.axis_size("ep")
    me = lax.axis_index("ep")
    _, _, my_z, _ = place()
    steps, row_count, width = tokens.shape
    capacity = 2
    tops = route_ids.shape[2]
    hidden_units = expert_in.shape[3]
    units = hidden_units // engines
    columns = width // engines
    numbers = jnp.arange(experts, dtype=jnp.int32)
    z_groups = [[x * ZS * CS + z * CS + c for z in range(ZS)] for x in range(XS) for c in range(CS)]
    pairs_xc = [(x, c) for x in range(XS) for c in range(CS)]
    xc_groups = [[x * ZS * CS + z * CS + c for x, c in pairs_xc] for z in range(ZS)]

    same = route_ids[:, :, None, :, None] == route_ids[:, None, :, None, :]
    earlier = jnp.arange(row_count)[:, None] > jnp.arange(row_count)[None, :]
    before = jnp.sum((same & earlier[None, :, :, None, None]).astype(jnp.int32), axis=(2, 4))
    marks = (route_ids * capacity + before).astype(jnp.bfloat16)
    notes = jnp.concatenate([marks] + exact_parts(route_weights), axis=2)
    notes = jnp.pad(notes, ((0, 0), (0, 0), (0, 128 - 4 * tops)))
    payload = jnp.concatenate([tokens, notes], axis=2).reshape(steps * row_count, -1)
    column = lax.all_gather(payload, "ep", axis_index_groups=z_groups, axis=0, tiled=False)
    everyone = lax.all_gather(column, "ep", axis_index_groups=xc_groups, axis=0, tiled=False)
    parts = jnp.concatenate([expert_in[..., e * units : (e + 1) * units] for e in range(engines)], axis=0)
    held_in = lax.all_to_all(parts, BOTH, split_axis=0, concat_axis=0, tiled=True)
    held_down = lax.all_to_all(
        jnp.transpose(expert_down, (0, 2, 1)), "ep", split_axis=0, concat_axis=0, tiled=True
    )
    held_down = held_down.reshape(columns, hidden_units)

    marks = everyone[..., width : width + tops].reshape(peers, steps, row_count, tops)
    first = (me * capacity).astype(jnp.bfloat16)
    slot = jnp.where(jnp.any(marks == first, axis=3), 0, jnp.where(jnp.any(marks == first + 1, axis=3), 1, -1))
    number = jnp.arange(CS * XS, dtype=jnp.int32)
    near_x, near_c = number // CS, number % CS
    base = ((near_c * XS + near_x)[:, None] * ZS + jnp.arange(ZS, dtype=jnp.int32)).reshape(peers, 1, 1) * capacity
    codes = jnp.where(slot >= 0, base + slot, -1)
    slots = jnp.arange(peers * capacity, dtype=jnp.int32)
    notes = column[..., width : width + 4 * tops].reshape(-1, width)
    notes = jnp.pad(notes, ((0, 8 - notes.shape[0]), (0, 0)))
    all_rows = everyone.reshape(-1, everyone.shape[-1])
    turn = jnp.arange(steps, dtype=jnp.int32)[None, :, None]
    gathered = []
    for step in range(steps):
        chosen = (slots[:, None] == jnp.where(turn == step, codes, -1).reshape(-1)[None, :]).astype(jnp.bfloat16)
        arrived = jnp.dot(chosen, all_rows, preferred_element_type=jnp.float32).astype(jnp.bfloat16)[:, :width]
        gathered.append(lax.all_gather(jnp.concatenate([arrived, notes]), "engine", axis=0, tiled=False))

    notes = gathered[0][:, peers * capacity].reshape(YS, ZS, steps, row_count, 4 * tops)
    notes = jnp.transpose(notes, (2, 1, 0, 3, 4)).reshape(steps, ZS * YS * row_count, 4, tops).astype(jnp.float32)
    marks, strength = notes[:, :, 0], notes[:, :, 1] + notes[:, :, 2] + notes[:, :, 3]
    block = jnp.arange(ZS * YS * row_count, dtype=jnp.int32) // row_count
    block = ((block % YS) * ZS + block // YS) * capacity
    lanes = jnp.arange(CS * XS * YS * ZS * capacity, dtype=jnp.int32)
    near = jnp.arange(CS * XS, dtype=jnp.int32)
    target = (((near % XS) * (ZS * CS) + my_z * CS + near // XS) * capacity).astype(jnp.float32)
    lower = marks[..., None] == target
    upper = marks[..., None] == target + 1.0
    share = jnp.sum(jnp.where(lower | upper, strength[..., None], 0.0), axis=2)
    spot = block[:, None] + near * (YS * ZS * capacity) + jnp.any(upper, axis=2).astype(jnp.int32)
    mixing = sum(jnp.where(spot[:, :, n, None] == lanes, share[:, :, n, None], 0.0) for n in range(CS * XS))

    top = jnp.max(jnp.abs(held_in), axis=(0, 2)).astype(jnp.float32)
    scale_in = (top + EPSILON) / quant_levels
    quant_in = jnp.floor(held_in.astype(jnp.float32) / scale_in[None, :, None, :] + 0.5).astype(jnp.bfloat16)
    quant_in = jnp.transpose(quant_in, (1, 0, 2, 3)).reshape(2, width, units)
    hidden = []
    for step in range(steps):
        rows = gathered[step].reshape(-1, width)
        projected = jnp.einsum("nd,mdf->mnf", rows, quant_in, preferred_element_type=jnp.float32)
        projected = projected * scale_in[:, None, :]
        part = (jax.nn.silu(projected[0]) * projected[1]).astype(jnp.bfloat16)
        part = lax.all_gather(part, "engine", axis=0, tiled=False)
        hidden.append(jnp.concatenate([part[e] for e in range(engines)], axis=-1))
    hidden = jnp.concatenate(hidden)

    scale_out = (jnp.max(jnp.abs(held_down), axis=1).astype(jnp.float32) + EPSILON) / quant_levels
    quant_down = jnp.floor(held_down.astype(jnp.float32) / scale_out[:, None] + 0.5).astype(jnp.bfloat16)
    summed = jnp.einsum("nf,cf->nc", hidden, quant_down, preferred_element_type=jnp.float32)
    outcome = (summed * scale_out).astype(jnp.bfloat16)
    outcome = outcome.reshape(steps, YS, -1, columns)
    scales = jnp.concatenate([scale_in.reshape(-1), scale_out, jnp.zeros((256,), jnp.float32)]).reshape(16, 128)
    combined, heard = give_back(outcome, mixing, scales, row_count, ZS * capacity)
    mine = jnp.sum(jnp.where(placement == me, numbers, 0))
    spot = ((mine % CS) * XS + mine // (ZS * CS)) * ZS + (mine // CS) % ZS
    picked = lax.dynamic_index_in_dim(heard.reshape(experts, -1), spot, 0, keepdims=False)
    in_scales = picked[: 2 * units].reshape(1, 2, units)
    out_scales = picked[2 * units : 2 * units + columns].reshape(1, columns)
    return (combined.reshape(steps, row_count, width), in_scales, out_scales)


def solution(mesh):
    placed = (
        P(None, ("engine", "ep"), None),
        P(None, ("engine", "ep"), None),
        P(None, ("engine", "ep"), None),
        P(),
        P(None, None, ("engine", "ep"), None),
        P(None, None, ("engine", "ep")),
    )
    return jax.shard_map(
        layer,
        mesh=mesh,
        in_specs=placed,
        out_specs=(P(None, ("engine", "ep"), None), P("ep", None, "engine"), P("ep", "engine")),
        check_vma=False,
    )
```

```python
import jax
import jax.numpy as jnp
from jax import lax
from jax.experimental import pallas as pl
from jax.experimental.pallas import tpu as pltpu
from jax.sharding import PartitionSpec as P


EPSILON = 1e-06
quant_levels = 31.0
BOTH = ("engine", "ep")
MESH = pl.DeviceIdType.MESH
XS, ZS, CS, YS = 4, 8, 2, 4


def place():
    p = lax.axis_index("ep")
    return lax.axis_index("engine"), p // (ZS * CS), (p // CS) % ZS, p % CS


def device(y, x, z, c):
    return {"engine": y, "ep": x * (ZS * CS) + z * CS + c}


def peers_of(kind):
    y, x, z, c = place()
    if kind == "z":
        return [device(y, x, (z + d) % ZS, c) for d in (4, 3, 5, 2, 6, 1, 7)]
    if kind == "x":
        return [device(y, (x + d) % XS, z, c) for d in (2, 1, 3)]
    if kind == "y":
        return [device((y + d) % YS, x, z, c) for d in (2, 1, 3)]
    if kind == "c":
        return [device(y, x, z, 1 - c)]
    return [device(y, (x + d) % XS, z, (c + f) % CS) for f in (0, 1) for d in range(XS) if (d, f) != (0, 0)]


def greet(kinds):
    barrier = pltpu.get_barrier_semaphore()
    count = 0
    for kind in kinds:
        for peer in peers_of(kind):
            pl.semaphore_signal(barrier, inc=1, device_id=peer, device_id_type=MESH)
            count += 1
    pl.semaphore_wait(barrier, count)


def send(src, dst, send_sem, recv_sem, peer):
    copy = pltpu.make_async_remote_copy(
        src_ref=src, dst_ref=dst, send_sem=send_sem, recv_sem=recv_sem, device_id=peer, device_id_type=MESH
    )
    copy.start()
    return copy


def await_bytes(like, sem):
    pltpu.make_async_copy(like, like, sem).wait()


def return_kernel(outcome, mixing, scales, out, heard, first, partial, second, total, third, sent, got, own):
    steps, halves, block, part = mixing.shape[0], first.shape[0], first.shape[4], first.shape[5]
    y, x, z, c = place()
    here = c * XS + x
    note = 2 * steps * halves
    chunks = [(h, s) for h in range(halves) for s in range(steps)]

    def rows_for(h, s, peer):
        start = pl.multiple_of((s * CS * XS + peer) * block, block)
        return outcome.at[:, pl.ds(start, block), pl.ds(h * part, part)]

    greet(("xc", "z", "y"))
    heard[here, z] = scales[...]
    own_copies = []
    for k, (h, s) in enumerate(chunks):
        own_copies.append(pltpu.make_async_copy(rows_for(h, s, here), first.at[h, s, here], own.at[k]))
        own_copies[k].start()
        for f, d in ((0, 2), (1, 2), (0, 1), (0, 3), (1, 1), (1, 3), (1, 0)):
            there_x, there_c = (x + d) % XS, (c + f) % CS
            src = rows_for(h, s, there_c * XS + there_x)
            send(src, first.at[h, s, here], sent.at[k], got.at[k], device(y, there_x, z, there_c))
        if k == 0:
            for f, d in ((0, 2), (0, 1), (0, 3), (1, 2), (1, 1), (1, 3), (1, 0)):
                peer = device(y, (x + d) % XS, z, (c + f) % CS)
                send(scales, heard.at[here, z], sent.at[note], got.at[note], peer)
    for k, (h, s) in enumerate(chunks):
        own_copies[k].wait()
        await_bytes(first.at[h, s, pl.ds(0, XS * CS - 1)], got.at[k])
        rows = first[h, s].reshape(-1, part).astype(jnp.float32)
        sums = jnp.dot(mixing[s], rows, precision=lax.Precision.HIGHEST, preferred_element_type=jnp.float32)
        partial[h, s] = sums.astype(partial.dtype).reshape(partial.shape[2:])
        second[h, s, z] = partial[h, s, z]
        for d in (4, 3, 5, 2, 6, 1, 7):
            there = (z + d) % ZS
            pair = note + 3 + k
            send(partial.at[h, s, there], second.at[h, s, z], sent.at[pair], got.at[pair], device(y, x, there, c))
        if k == 0:
            await_bytes(heard.at[pl.ds(0, XS * CS - 1), z], got.at[note])
            for peer in peers_of("z"):
                send(heard.at[:, z], heard.at[:, z], sent.at[note + 1], got.at[note + 1], peer)
    for h in range(halves):
        sums = []
        for s in range(steps):
            await_bytes(second.at[h, s, pl.ds(0, ZS - 1)], got.at[note + 3 + h * steps + s])
            sums.append(jnp.sum(second[h, s].astype(jnp.float32), axis=0).reshape(YS, -1, part))
        total[h] = jnp.concatenate(sums, axis=1).astype(total.dtype)
        third[h, y] = total[h, y]
        for d in (2, 1, 3):
            there = (y + d) % YS
            last = steps * halves + h
            send(total.at[h, there], third.at[h, y], sent.at[last], got.at[last], device(there, x, z, c))
    for h in range(halves):
        await_bytes(third.at[h, pl.ds(0, YS - 1)], got.at[steps * halves + h])
        for e in range(YS):
            start = (e * halves + h) * part
            out[:, start : start + part] = third[h, e]
    await_bytes(heard.at[:, pl.ds(0, ZS - 1)], got.at[note + 1])
    await_bytes(heard.at[pl.ds(0, XS * CS - 1), z], sent.at[note])
    await_bytes(heard.at[:, pl.ds(0, ZS - 1)], sent.at[note + 1])
    for k, (h, s) in enumerate(chunks):
        await_bytes(first.at[h, s, pl.ds(0, XS * CS - 1)], sent.at[k])
        await_bytes(second.at[h, s, pl.ds(0, ZS - 1)], sent.at[note + 3 + k])
    for h in range(halves):
        await_bytes(third.at[h, pl.ds(0, YS - 1)], sent.at[steps * halves + h])


def give_back(outcome, mixing, scales, row_count, block, halves=2):
    steps, columns = mixing.shape[0], outcome.shape[-1]
    part = columns // halves
    vmem = pl.BlockSpec(memory_space=pltpu.VMEM)
    kept = outcome.dtype
    count = 3 * steps * halves + 3
    return pl.pallas_call(
        return_kernel,
        out_shape=(
            jax.ShapeDtypeStruct((steps * row_count, YS * columns), kept),
            jax.ShapeDtypeStruct((XS * CS, ZS) + scales.shape, scales.dtype),
        ),
        in_specs=[pl.BlockSpec(memory_space=pl.ANY), vmem, vmem],
        out_specs=(vmem, vmem),
        scratch_shapes=[
            pltpu.VMEM((halves, steps, CS * XS, YS, block, part), kept),
            pltpu.VMEM((halves, steps, ZS, YS * row_count, part), kept),
            pltpu.VMEM((halves, steps, ZS, YS * row_count, part), kept),
            pltpu.VMEM((halves, YS, steps * row_count, part), kept),
            pltpu.VMEM((halves, YS, steps * row_count, part), kept),
            pltpu.SemaphoreType.DMA((count,)),
            pltpu.SemaphoreType.DMA((count,)),
            pltpu.SemaphoreType.DMA((steps * halves,)),
        ],
        compiler_params=pltpu.CompilerParams(
            collective_id=0, has_side_effects=True, vmem_limit_bytes=48 * 1024 * 1024
        ),
        cost_estimate=pl.CostEstimate(flops=20_000_000_000, bytes_accessed=10_000_000, transcendentals=0),
        name="give_back",
    )(outcome, mixing, scales)


def exact_parts(values):
    high = lax.reduce_precision(values, 8, 7)
    middle = lax.reduce_precision(values - high, 8, 7)
    return [part.astype(jnp.bfloat16) for part in (high, middle, values - high - middle)]


def layer(tokens, route_ids, route_weights, placement, expert_in, expert_down):
    experts = placement.shape[0]
    engines = lax.axis_size("engine")
    peers = lax.axis_size("ep")
    me = lax.axis_index("ep")
    _, _, my_z, _ = place()
    steps, row_count, width = tokens.shape
    capacity = 2
    tops = route_ids.shape[2]
    hidden_units = expert_in.shape[3]
    units = hidden_units // engines
    columns = width // engines
    numbers = jnp.arange(experts, dtype=jnp.int32)
    z_groups = [[x * ZS * CS + z * CS + c for z in range(ZS)] for x in range(XS) for c in range(CS)]
    xc_groups = [[x * ZS * CS + z * CS + c for c in range(CS) for x in range(XS)] for z in range(ZS)]

    same = route_ids[:, :, None, :, None] == route_ids[:, None, :, None, :]
    earlier = jnp.arange(row_count)[:, None] > jnp.arange(row_count)[None, :]
    before = jnp.sum((same & earlier[None, :, :, None, None]).astype(jnp.int32), axis=(2, 4))
    marks = (route_ids * capacity + before).astype(jnp.bfloat16)
    notes = jnp.concatenate([marks] + exact_parts(route_weights), axis=2)
    notes = jnp.pad(notes, ((0, 0), (0, 0), (0, 128 - 4 * tops)))
    payload = jnp.concatenate([tokens, notes], axis=2).reshape(steps * row_count, -1)
    column = lax.all_gather(payload, "ep", axis_index_groups=z_groups, axis=0, tiled=False)
    everyone = lax.all_gather(column, "ep", axis_index_groups=xc_groups, axis=0, tiled=False)
    parts = jnp.concatenate([expert_in[..., e * units : (e + 1) * units] for e in range(engines)], axis=0)
    held_in = lax.all_to_all(parts, BOTH, split_axis=0, concat_axis=0, tiled=True)
    held_down = lax.all_to_all(
        jnp.transpose(expert_down, (0, 2, 1)), "ep", split_axis=0, concat_axis=0, tiled=True
    )
    held_down = held_down.reshape(columns, hidden_units)

    marks = everyone[..., width : width + tops].reshape(peers, steps, row_count, tops)
    first = (me * capacity).astype(jnp.bfloat16)
    slot = jnp.where(jnp.any(marks == first, axis=3), 0, jnp.where(jnp.any(marks == first + 1, axis=3), 1, -1))
    base = jnp.arange(peers, dtype=jnp.int32)[:, None, None] * capacity
    base = base + jnp.arange(steps, dtype=jnp.int32)[None, :, None] * (peers * capacity)
    codes = jnp.where(slot >= 0, base + slot, -1).reshape(-1)
    slots = jnp.arange(steps * peers * capacity, dtype=jnp.int32)
    chosen = (slots[:, None] == codes[None, :]).astype(jnp.bfloat16)
    arrived = jnp.dot(
        chosen, everyone.reshape(-1, everyone.shape[-1]), preferred_element_type=jnp.float32
    ).astype(jnp.bfloat16)[:, :width]
    notes = column[..., width : width + 4 * tops].reshape(-1, width)
    notes = jnp.pad(notes, ((0, 8 - notes.shape[0]), (0, 0)))
    gathered = lax.all_gather(jnp.concatenate([arrived, notes]), "engine", axis=0, tiled=False)
    row_total = arrived.shape[0]

    notes = gathered[:, row_total].reshape(YS, ZS, steps, row_count, 4 * tops)
    notes = jnp.transpose(notes, (2, 1, 0, 3, 4)).reshape(steps, ZS * YS * row_count, 4, tops).astype(jnp.float32)
    marks, strength = notes[:, :, 0], notes[:, :, 1] + notes[:, :, 2] + notes[:, :, 3]
    block = jnp.arange(ZS * YS * row_count, dtype=jnp.int32) // row_count
    block = ((block % YS) * ZS + block // YS) * capacity
    lanes = jnp.arange(CS * XS * YS * ZS * capacity, dtype=jnp.int32)
    near = jnp.arange(CS * XS, dtype=jnp.int32)
    target = (((near % XS) * (ZS * CS) + my_z * CS + near // XS) * capacity).astype(jnp.float32)
    lower = marks[..., None] == target
    upper = marks[..., None] == target + 1.0
    share = jnp.sum(jnp.where(lower | upper, strength[..., None], 0.0), axis=2)
    spot = block[:, None] + near * (YS * ZS * capacity) + jnp.any(upper, axis=2).astype(jnp.int32)
    mixing = sum(jnp.where(spot[:, :, n, None] == lanes, share[:, :, n, None], 0.0) for n in range(CS * XS))

    top = jnp.max(jnp.abs(held_in), axis=(0, 2)).astype(jnp.float32)
    scale_in = (top + EPSILON) / quant_levels
    quant_in = jnp.floor(held_in.astype(jnp.float32) / scale_in[None, :, None, :] + 0.5).astype(jnp.bfloat16)
    quant_in = jnp.transpose(quant_in, (1, 0, 2, 3)).reshape(2, width, units)
    rows = gathered.reshape(-1, width)
    projected = jnp.einsum("nd,mdf->mnf", rows, quant_in, preferred_element_type=jnp.float32)
    projected = projected * scale_in[:, None, :]
    hidden = (jax.nn.silu(projected[0]) * projected[1]).astype(jnp.bfloat16)
    hidden = lax.all_gather(hidden, "engine", axis=0, tiled=False)
    hidden = jnp.concatenate([hidden[e] for e in range(engines)], axis=-1)

    scale_out = (jnp.max(jnp.abs(held_down), axis=1).astype(jnp.float32) + EPSILON) / quant_levels
    quant_down = jnp.floor(held_down.astype(jnp.float32) / scale_out[:, None] + 0.5).astype(jnp.bfloat16)
    summed = jnp.einsum("nf,cf->nc", hidden, quant_down, preferred_element_type=jnp.float32)
    outcome = (summed * scale_out).astype(jnp.bfloat16)
    outcome = outcome.reshape(YS, -1, columns)
    scales = jnp.concatenate([scale_in.reshape(-1), scale_out, jnp.zeros((256,), jnp.float32)]).reshape(16, 128)
    combined, heard = give_back(outcome, mixing, scales, row_count, ZS * capacity)
    mine = jnp.sum(jnp.where(placement == me, numbers, 0))
    spot = ((mine % CS) * XS + mine // (ZS * CS)) * ZS + (mine // CS) % ZS
    picked = lax.dynamic_index_in_dim(heard.reshape(experts, -1), spot, 0, keepdims=False)
    in_scales = picked[: 2 * units].reshape(1, 2, units)
    out_scales = picked[2 * units : 2 * units + columns].reshape(1, columns)
    return (combined.reshape(steps, row_count, width), in_scales, out_scales)


def solution(mesh):
    placed = (
        P(None, ("engine", "ep"), None),
        P(None, ("engine", "ep"), None),
        P(None, ("engine", "ep"), None),
        P(),
        P(None, None, ("engine", "ep"), None),
        P(None, None, ("engine", "ep")),
    )
    return jax.shard_map(
        layer,
        mesh=mesh,
        in_specs=placed,
        out_specs=(P(None, ("engine", "ep"), None), P("ep", None, "engine"), P("ep", "engine")),
        check_vma=False,
    )
```
